16 devices in a mesh: tp: 2 (over z), ep: 8 (over y, x, core).
Axes of the slice: x: 2, y: 2, z: 2, core: 2. Of those that a mesh axis runs over, the one named last changes fastest.
Arguments:
- x: bfloat16 [2048, 1536], P(('ep', 'tp'))
- grad_y: bfloat16 [2048, 1536], P(('ep', 'tp'))
- w_router: bfloat16 [1536, 64], replicated
- w_gate: bfloat16 [64, 1536, 512], P('ep', None, 'tp')
- w_up: bfloat16 [64, 1536, 512], P('ep', None, 'tp')
- w_down: bfloat16 [64, 512, 1536], P('ep', 'tp')
- ws_gate: bfloat16 [1536, 1024], P(None, 'tp')
- ws_up: bfloat16 [1536, 1024], P(None, 'tp')
- ws_down: bfloat16 [1024, 1536], P('tp')
- topk_idx: int32 [2048, 6], P(('ep', 'tp'))
Outputs:
- output 1: bfloat16 [2048, 1536], P(('ep', 'tp'))
- output 2: bfloat16 [2048, 1536], P(('ep', 'tp'))
- output 3: float32 [1536, 64], replicated
- output 4: float32 [64, 1536, 512], P('ep', None, 'tp')
- output 5: float32 [64, 1536, 512], P('ep', None, 'tp')
- output 6: float32 [64, 512, 1536], P('ep', 'tp')
- output 7: float32 [1536, 1024], P(None, 'tp')
- output 8: float32 [1536, 1024], P(None, 'tp')
- output 9: float32 [1024, 1536], P('tp')
All inputs are finite; a program needn't handle non-finite values.
Results may differ from the reference program's by a relative error of at most 0.0130894.
Values are sent between devices in bfloat16 or wider.
A program may use at most 1 GiB of HBM per device.

```python
import jax
import jax.numpy as jnp
from jax import lax

D = 1536
EXPERTS = 64
FF = 512
SHARED_FF = 1024
TOP = 6
TOK = 128
TP = 2
EP = 8

GATE_SCALE = 16.0


def capacity():
    groups = TOP // 2
    most = groups * TOK // (2 * EP) + min(groups, EP // 2) * TOK // EP
    per_group = EXPERTS // EP
    return (2 * most + per_group - 1) // per_group


def draw_routes(key):
    devices = TP * EP
    groups = TOP // 2
    half_tok = TOK // 2
    per_group = EXPERTS // EP
    role_key, group_key, local_key = jax.random.split(key, 3)
    role_ids = jax.vmap(lambda sub_key: jax.random.permutation(sub_key, TOK))(jax.random.split(role_key, devices))
    base_group = jnp.where(role_ids < half_tok, role_ids % EP, role_ids % (EP // 2))
    visited = (base_group[:, :, None] + jnp.arange(groups)[None, None, :]) % EP
    hit_map = jax.nn.one_hot(visited.reshape(devices, TOK * groups), EP, dtype=jnp.int32)
    visit_num = jnp.sum((jnp.cumsum(hit_map, axis=1) - hit_map) * hit_map, axis=2).reshape(devices, TOK, groups)
    local_ids = (2 * visit_num[:, :, :, None] + jnp.arange(2)[None, None, None, :]) % per_group
    group_perm = jax.vmap(lambda sub_key: jax.random.permutation(sub_key, EP))(jax.random.split(group_key, devices))
    local_perm = jax.vmap(lambda sub_key: jax.random.permutation(sub_key, per_group))(jax.random.split(local_key, devices * EP)).reshape(devices, EP * per_group)
    true_group = jnp.take_along_axis(group_perm, visited.reshape(devices, TOK * groups), axis=1).reshape(devices, TOK, groups, 1)
    position = (true_group * per_group + local_ids).reshape(devices, TOK * TOP)
    local_pick = jnp.take_along_axis(local_perm, position, axis=1).reshape(devices, TOK, groups, 2)
    expert_ids = true_group * per_group + local_pick
    return expert_ids.reshape(devices * TOK, TOP).astype(jnp.int32)


def normal_bf16(key, arr_shape, std_dev):
    return (jax.random.normal(key, arr_shape, jnp.float32) * std_dev).astype(jnp.bfloat16)


def setup_inputs(seed: int = 0) -> dict:
    key_list = jax.random.split(jax.random.key(seed), 10)
    tokens = TOK * TP * EP
    return dict(
        x=normal_bf16(key_list[0], (tokens, D), 1.0),
        grad_y=normal_bf16(key_list[1], (tokens, D), 1.0),
        w_router=normal_bf16(key_list[2], (D, EXPERTS), D ** -0.5),
        w_gate=normal_bf16(key_list[3], (EXPERTS, D, FF), D ** -0.5),
        w_up=normal_bf16(key_list[4], (EXPERTS, D, FF), D ** -0.5),
        w_down=normal_bf16(key_list[5], (EXPERTS, FF, D), FF ** -0.5),
        ws_gate=normal_bf16(key_list[6], (D, SHARED_FF), D ** -0.5),
        ws_up=normal_bf16(key_list[7], (D, SHARED_FF), D ** -0.5),
        ws_down=normal_bf16(key_list[8], (SHARED_FF, D), SHARED_FF ** -0.5),
        topk_idx=draw_routes(key_list[9]),
    )


def swiglu(rows_in, w_a, w_b, w_c):
    gate_pre = jnp.dot(rows_in, w_a).astype(jnp.bfloat16).astype(jnp.float32)
    up_pre = jnp.dot(rows_in, w_b).astype(jnp.bfloat16).astype(jnp.float32)
    hidden = (jax.nn.silu(gate_pre) * up_pre).astype(jnp.bfloat16).astype(jnp.float32)
    return jnp.dot(hidden, w_c)


def reference(x, grad_y, w_router, w_gate, w_up, w_down, ws_gate, ws_up, ws_down, topk_idx):
    tokens = x.shape[0]
    cap_all = capacity() * TP * EP
    hit_count = jnp.sum(jax.nn.one_hot(topk_idx, EXPERTS, dtype=jnp.int32), axis=1)
    slot_rank = jnp.cumsum(hit_count, axis=0) - hit_count
    slot_of = topk_idx * cap_all + jnp.take_along_axis(slot_rank, topk_idx, axis=1)
    token_ids = jnp.broadcast_to(jnp.arange(tokens, dtype=jnp.int32)[:, None], slot_of.shape)
    slot_owner = jnp.zeros((EXPERTS * cap_all,), jnp.int32).at[slot_of.reshape(-1)].set(token_ids.reshape(-1)).reshape(EXPERTS, cap_all)

    def forward(x_wide, router_w, gate_w, up_w, down_w, sgate_w, sup_w, sdown_w):
        router_probs = jax.nn.softmax(jnp.dot(x_wide, router_w), axis=-1)
        route_gates = GATE_SCALE * jnp.take_along_axis(router_probs, topk_idx, axis=1)
        total = swiglu(x_wide, sgate_w, sup_w, sdown_w)

        def one_expert(operands):
            owner_ids, w_a, w_b, w_c = operands
            expert_rows = jnp.take(x_wide, owner_ids, axis=0).astype(jnp.bfloat16).astype(jnp.float32)
            return swiglu(expert_rows, w_a, w_b, w_c).astype(jnp.bfloat16)

        expert_out = lax.map(jax.checkpoint(one_expert), (slot_owner, gate_w, up_w, down_w)).reshape(EXPERTS * cap_all, D)
        for k in range(TOP):
            total = total + route_gates[:, k:k + 1] * jnp.take(expert_out, slot_of[:, k], axis=0).astype(jnp.float32)
        return total.astype(jnp.bfloat16)

    y_out, pullback = jax.vjp(forward, x.astype(jnp.float32), w_router.astype(jnp.float32), w_gate.astype(jnp.float32), w_up.astype(jnp.float32), w_down.astype(jnp.float32), ws_gate.astype(jnp.float32), ws_up.astype(jnp.float32), ws_down.astype(jnp.float32))
    grads = pullback(grad_y)
    return (y_out, grads[0].astype(jnp.bfloat16), grads[1], grads[2], grads[3], grads[4], grads[5], grads[6], grads[7])
```

```python
import jax
import jax.numpy as jnp
from jax import lax
from jax.sharding import PartitionSpec as P

GATE_SCALE = 16.0
BF = jnp.bfloat16
F32 = jnp.float32
COL_CHUNKS = 3


def swiglu_act(gate_pre, up_pre):
    return jax.nn.silu(gate_pre) * up_pre


def act_grads(gate_pre, up_pre, d_hidden):
    _, vjp = jax.vjp(swiglu_act, gate_pre.astype(F32), up_pre.astype(F32))
    d_gate, d_up = vjp(d_hidden.astype(F32))
    return d_gate.astype(BF), d_up.astype(BF)


def dot(spec, a, b):
    return jnp.einsum(spec, a, b, preferred_element_type=F32)


def three_parts(v):
    hi = lax.reduce_precision(v, 8, 7)
    rest = v - hi
    mid = lax.reduce_precision(rest, 8, 7)
    low = lax.reduce_precision(rest - mid, 8, 7)
    return hi.astype(BF), mid.astype(BF), low.astype(BF)


def solution(mesh):
    tp_size = mesh.shape['tp']
    ep_size = mesh.shape['ep']
    devices = tp_size * ep_size
    swap = [(i, 1 - i) for i in range(tp_size)]

    def zswap(v):
        return lax.ppermute(v, 'tp', swap)

    def ep_swap(v, bit):
        return lax.ppermute(v, 'ep', [(i, i ^ bit) for i in range(ep_size)])

    def reduce_rows(v):
        me = lax.axis_index('ep')
        bits = (me // 4, (me // 2) % 2, me % 2)
        cols = v.shape[1]
        v = v.reshape(2, 2, 2, v.shape[0] // 8, cols)

        def halve(u, axis, which):
            mine = lax.dynamic_index_in_dim(u, bits[which], axis, keepdims=False)
            other = lax.dynamic_index_in_dim(u, 1 - bits[which], axis, keepdims=False)
            return mine + ep_swap(other, (4, 2, 1)[which])

        v = halve(v, 2, 2)
        left, right = v[..., :cols // 2], v[..., cols // 2:]
        left = halve(halve(left, 1, 1), 0, 0)
        right = halve(halve(right, 0, 0), 0, 1)
        return jnp.concatenate([left, right], axis=-1)

    def device_step(x, grad_y, w_router, w_gate, w_up, w_down, ws_gate, ws_up, ws_down, topk_idx):
        tok_rows, dim = x.shape
        top_k = topk_idx.shape[1]
        experts = w_router.shape[1]
        n_loc, _, ff = w_gate.shape
        sff = ws_gate.shape[1]
        groups = top_k // 2
        most = groups * tok_rows // (2 * ep_size) + min(groups, ep_size // 2) * tok_rows // ep_size
        cap = (2 * most + n_loc - 1) // n_loc
        tokens = tok_rows * devices
        half = dim // 2
        me = lax.axis_index('ep')
        z = lax.axis_index('tp')
        my_col, other_col = z * half, (1 - z) * half

        w2_give = lax.dynamic_slice_in_dim(w_down, other_col, half, 2)
        w2_other = zswap(w2_give)
        idx_all = lax.all_gather(topk_idx, ('ep', 'tp'), axis=0, tiled=True)
        x_all = lax.all_gather(x, ('ep', 'tp'), axis=0, tiled=True)
        dy_all = lax.all_gather(grad_y, ('ep', 'tp'), axis=0, tiled=True)

        local_ids = me * n_loc + jnp.arange(n_loc, dtype=jnp.int32)
        mine = jnp.sum((idx_all[:, :, None] == local_ids[None, None, :]).astype(jnp.int32), axis=1)
        mine_dev = mine.reshape(devices, tok_rows, n_loc)
        before = jnp.tril(jnp.ones((tok_rows, tok_rows), BF), -1)
        rank = jnp.einsum('ut,dte->due', before, mine_dev.astype(BF), preferred_element_type=F32).astype(jnp.int32)
        per_half = devices // 2
        slot = (jnp.arange(devices, dtype=jnp.int32) % per_half)[:, None, None] * cap + rank
        slot = jnp.where(mine_dev > 0, slot, -1).reshape(2, per_half * tok_rows, n_loc)
        n_slot = per_half * cap
        pick = jnp.arange(n_slot, dtype=jnp.int32)[None, None, :, None] == slot.transpose(0, 2, 1)[:, :, None, :]
        sel = pick.astype(BF)

        logits = jnp.dot(x_all, w_router, preferred_element_type=F32)
        probs = jax.nn.softmax(logits, axis=-1)
        gate_loc = GATE_SCALE * lax.dynamic_slice_in_dim(probs, me * n_loc, n_loc, 1)
        gate_t = gate_loc.reshape(2, per_half * tok_rows, n_loc).transpose(0, 2, 1)
        gate_slot = jnp.sum(jnp.where(pick, gate_t[:, :, None, :], 0.0), axis=-1)

        x_half = x_all.reshape(2, per_half * tok_rows, dim)
        dy_half = dy_all.reshape(2, per_half * tok_rows, dim)
        rows = dot('hest,htd->hesd', sel, x_half).astype(BF)
        dy_rows = dot('hest,htd->hesd', sel, dy_half).astype(BF)
        d_out = (dy_rows.astype(F32) * gate_slot[..., None]).astype(BF)

        gate_pre = dot('hesd,edf->hesf', rows, w_gate).astype(BF)
        up_pre = dot('hesd,edf->hesf', rows, w_up).astype(BF)
        hidden = swiglu_act(gate_pre.astype(F32), up_pre.astype(F32)).astype(BF)
        hidden_other = zswap(hidden)
        d_hidden = dot('hesd,efd->hesf', d_out, w_down).astype(BF)
        d_gate_pre, d_up_pre = act_grads(gate_pre, up_pre, d_hidden)

        w1_other = lax.dynamic_slice_in_dim(w_gate, other_col, half, 1)
        w3_other = lax.dynamic_slice_in_dim(w_up, other_col, half, 1)
        w1_mine = lax.dynamic_slice_in_dim(w_gate, my_col, half, 1)
        w3_mine = lax.dynamic_slice_in_dim(w_up, my_col, half, 1)
        width = half // COL_CHUNKS
        dx_parts = []
        for j in range(COL_CHUNKS):
            c = slice(j * width, (j + 1) * width)
            give = dot('hesf,edf->hesd', d_gate_pre, w1_other[:, c]) + dot('hesf,edf->hesd', d_up_pre, w3_other[:, c])
            got = zswap(give)
            own = dot('hesf,edf->hesd', d_gate_pre, w1_mine[:, c]) + dot('hesf,edf->hesd', d_up_pre, w3_mine[:, c])
            d_rows = (own + got).astype(BF)
            dense = dot('hest,hesd->htd', sel, d_rows).reshape(tokens, width)
            dx_parts.append(reduce_rows(dense))
        dx_routed = jnp.concatenate(dx_parts, axis=1)

        w2_mine = lax.dynamic_slice_in_dim(w_down, my_col, half, 2)
        out_rows = (dot('hesf,efd->hesd', hidden, w2_mine) + dot('hesf,efd->hesd', hidden_other, w2_other)).astype(BF)
        dy_mine = lax.dynamic_slice_in_dim(dy_rows, my_col, half, 3)
        d_gate_slot = jnp.sum(out_rows.astype(F32) * dy_mine.astype(F32), axis=-1)
        d_gate_t = jnp.sum(jnp.where(pick, d_gate_slot[..., None], 0.0), axis=2).transpose(0, 2, 1).reshape(tokens, n_loc)
        d_gate_wide = lax.dynamic_update_slice_in_dim(jnp.zeros((tokens, experts), F32), d_gate_t, me * n_loc, 1)
        scaled = out_rows.astype(F32) * gate_slot[..., None]
        hi, mid, low = three_parts(scaled)
        y_dense = dot('hest,hesd->htd', sel, hi) + dot('hest,hesd->htd', sel, mid) + dot('hest,hesd->htd', sel, low)
        y_sum = reduce_rows(y_dense.reshape(tokens, half))
        dg_sum = reduce_rows(d_gate_wide)
        d_gates = dg_sum + zswap(dg_sum)

        sg_pre = jnp.dot(x_all, ws_gate, preferred_element_type=F32).astype(BF)
        su_pre = jnp.dot(x_all, ws_up, preferred_element_type=F32).astype(BF)
        s_hidden = swiglu_act(sg_pre.astype(F32), su_pre.astype(F32)).astype(BF)
        ds_hidden = dot('td,fd->tf', dy_all, ws_down).astype(BF)
        dsg_pre, dsu_pre = act_grads(sg_pre, su_pre, ds_hidden)
        ds_down = dot('tf,td->fd', s_hidden, dy_all)
        ds_gate = dot('td,tf->df', x_all, dsg_pre)
        ds_up = dot('td,tf->df', x_all, dsu_pre)
        grp = tp_size * tok_rows

        def own_rows(v):
            return lax.dynamic_slice_in_dim(v, me * grp, grp, 0)

        s_part = jnp.dot(own_rows(s_hidden), ws_down, preferred_element_type=F32)
        dxs_part = dot('tf,df->td', own_rows(dsg_pre), ws_gate) + dot('tf,df->td', own_rows(dsu_pre), ws_up)
        both = jnp.stack([s_part, dxs_part])
        got_shared = zswap(lax.dynamic_slice_in_dim(both, other_col, half, 2))
        shared = lax.dynamic_slice_in_dim(both, my_col, half, 2) + got_shared

        d_w_down = dot('hesf,hesd->efd', hidden, d_out)
        d_w_gate = dot('hesd,hesf->edf', rows, d_gate_pre)
        d_w_up = dot('hesd,hesf->edf', rows, d_up_pre)

        p_own = own_rows(probs)
        d_scores = GATE_SCALE * d_gates
        d_logits = p_own * (d_scores - jnp.sum(p_own * d_scores, axis=-1, keepdims=True))
        my_logits = lax.dynamic_slice_in_dim(d_logits, z * tok_rows, tok_rows, 0)
        d_router = lax.psum(dot('td,te->de', x, my_logits), ('tp', 'ep'))
        wr_mine = lax.dynamic_slice_in_dim(w_router, my_col, half, 0)
        dx_router = dot('te,de->td', d_logits, wr_mine)

        y_half = (shared[0] + y_sum).astype(BF)
        dx_half = (dx_router + shared[1] + dx_routed).astype(BF)
        outs = jnp.stack([y_half, dx_half]).reshape(2, tp_size, tok_rows, half)
        keep = lax.dynamic_index_in_dim(outs, z, 1, keepdims=False)
        got = zswap(lax.dynamic_index_in_dim(outs, 1 - z, 1, keepdims=False))
        full = jnp.where(z == 0, jnp.concatenate([keep, got], axis=-1), jnp.concatenate([got, keep], axis=-1))
        return full[0], full[1], d_router, d_w_gate, d_w_up, d_w_down, ds_gate, ds_up, ds_down

    tok_spec = P(('ep', 'tp'), None)
    in_specs = (tok_spec, tok_spec, P(None, None), P('ep', None, 'tp'), P('ep', None, 'tp'), P('ep', 'tp', None), P(None, 'tp'), P(None, 'tp'), P('tp', None), tok_spec)
    out_specs = (tok_spec, tok_spec, P(None, None), P('ep', None, 'tp'), P('ep', None, 'tp'), P('ep', 'tp', None), P(None, 'tp'), P(None, 'tp'), P('tp', None))
    return jax.shard_map(device_step, mesh=mesh, in_specs=in_specs, out_specs=out_specs, check_vma=False)
```

```python
import jax
import jax.numpy as jnp
from jax import lax
from jax.experimental import pallas as pl
from jax.experimental.pallas import tpu as pltpu
from jax.sharding import PartitionSpec as P

GATE_SCALE = 16.0
BF = jnp.bfloat16
F32 = jnp.float32
COL_CHUNKS = 3


def swiglu_act(gate_pre, up_pre):
    return jax.nn.silu(gate_pre) * up_pre


def act_grads(gate_pre, up_pre, d_hidden):
    _, vjp = jax.vjp(swiglu_act, gate_pre.astype(F32), up_pre.astype(F32))
    d_gate, d_up = vjp(d_hidden.astype(F32))
    return d_gate.astype(BF), d_up.astype(BF)


def dot(spec, a, b):
    return jnp.einsum(spec, a, b, preferred_element_type=F32)


def three_parts(v):
    hi = lax.reduce_precision(v, 8, 7)
    rest = v - hi
    mid = lax.reduce_precision(rest, 8, 7)
    low = lax.reduce_precision(rest - mid, 8, 7)
    return hi.astype(BF), mid.astype(BF), low.astype(BF)


def gather_kernel(own_ref, got_ref, out_ref, send_sem, recv_sem, local_sem):
    me = lax.axis_index('ep')
    z = lax.axis_index('tp')
    peers = {1: me + 1 - 2 * (me % 2), 2: me + 2 - 4 * ((me // 2) % 2), 4: me + 4 - 8 * (me // 4)}
    barrier = pltpu.get_barrier_semaphore()
    for bit in (1, 2, 4):
        pl.semaphore_signal(barrier, inc=1, device_id=(z, peers[bit]), device_id_type=pl.DeviceIdType.MESH)
    pl.semaphore_wait(barrier, 3)

    def send(src, block, part, bit):
        return pltpu.make_async_remote_copy(
            src_ref=src, dst_ref=out_ref.at[block, part], send_sem=send_sem.at[block, part],
            recv_sem=recv_sem.at[block, part], device_id=(z, peers[bit]), device_id_type=pl.DeviceIdType.MESH)

    locals_ = []
    sends = []
    for q, (ref, part) in enumerate(((own_ref, z), (got_ref, 1 - z))):
        for bit in (2, 4, 1):
            sends.append(send(ref, bit, part, bit))
            sends[-1].start()
        locals_.append(pltpu.make_async_copy(ref, out_ref.at[0, part], local_sem.at[q]))
        locals_[-1].start()

    def arrived(block, part):
        send(own_ref, block, part, 1).wait_recv()

    for part in (0, 1):
        arrived(2, part)
        if part == 0:
            sends.append(send(out_ref.at[2, 0], 6, 0, 4))
            sends[-1].start()
        sends.append(send(out_ref.at[2, part], 3, part, 1))
        sends[-1].start()
        arrived(4, part)
        if part == 1:
            sends.append(send(out_ref.at[4, 1], 6, 1, 2))
            sends[-1].start()
        sends.append(send(out_ref.at[4, part], 5, part, 1))
        sends[-1].start()
    for part in (0, 1):
        arrived(6, part)
        sends.append(send(out_ref.at[6, part], 7, part, 1))
        sends[-1].start()
    for block in (1, 3, 5, 7):
        for part in (0, 1):
            arrived(block, part)
    for copy in sends:
        copy.wait_send()
    for copy in locals_:
        copy.wait()


def gather_plane(own, got, collective_id):
    rows, dim = own.shape
    vmem = pl.BlockSpec(memory_space=pltpu.VMEM)
    return pl.pallas_call(
        gather_kernel,
        out_shape=jax.ShapeDtypeStruct((8, 2, rows, dim), own.dtype),
        in_specs=[vmem, vmem],
        out_specs=pl.BlockSpec(memory_space=pl.ANY),
        scratch_shapes=[pltpu.SemaphoreType.DMA((8, 2)), pltpu.SemaphoreType.DMA((8, 2)), pltpu.SemaphoreType.DMA((2,))],
        compiler_params=pltpu.CompilerParams(collective_id=collective_id, has_side_effects=True),
    )(own, got).reshape(16 * rows, dim)


def after(v, *earlier):
    return lax.optimization_barrier((v,) + earlier)[0]


def solution(mesh):
    tp_size = mesh.shape['tp']
    ep_size = mesh.shape['ep']
    devices = tp_size * ep_size
    swap = [(i, 1 - i) for i in range(tp_size)]

    def zswap(v):
        return lax.ppermute(v, 'tp', swap)

    def ep_swap(v, bit):
        return lax.ppermute(v, 'ep', [(i, i ^ bit) for i in range(ep_size)])

    def reduce_rows(v):
        cols = v.shape[1]
        v = v.reshape(2, 2, 2, v.shape[0] // 8, cols)
        v = v[:, :, 0] + ep_swap(v[:, :, 1], 1)
        left, right = v[..., :cols // 2], v[..., cols // 2:]
        left = left[:, 0] + ep_swap(left[:, 1], 2)
        right = right[0] + ep_swap(right[1], 4)
        left = left[0] + ep_swap(left[1], 4)
        right = right[0] + ep_swap(right[1], 2)
        return jnp.concatenate([left, right], axis=-1)

    def device_step(x, grad_y, w_router, w_gate, w_up, w_down, ws_gate, ws_up, ws_down, topk_idx):
        tok_rows, dim = x.shape
        top_k = topk_idx.shape[1]
        experts = w_router.shape[1]
        n_loc, _, ff = w_gate.shape
        groups = top_k // 2
        most = groups * tok_rows // (2 * ep_size) + min(groups, ep_size // 2) * tok_rows // ep_size
        cap = (2 * most + n_loc - 1) // n_loc
        tokens = tok_rows * devices
        grp = tp_size * tok_rows
        half = dim // 2
        me = lax.axis_index('ep')
        z = lax.axis_index('tp')
        my_col, other_col = z * half, (1 - z) * half

        x_got = zswap(x)
        dy_got = zswap(grad_y)
        idx = zswap(topk_idx)
        w2_other = zswap(lax.dynamic_slice_in_dim(w_down, other_col, half, 2))
        idx = jnp.where(z == 0, jnp.concatenate([topk_idx, idx]), jnp.concatenate([idx, topk_idx]))
        for bit in (1, 2, 4):
            idx = jnp.concatenate([idx, ep_swap(idx, bit)])
        x_all = gather_plane(x, x_got, 0)
        dy_all = gather_plane(grad_y, dy_got, 1)

        blocks = 4
        per_block = devices // blocks
        local_ids = me * n_loc + jnp.arange(n_loc, dtype=jnp.int32)
        mine = jnp.sum((idx[:, :, None] == local_ids[None, None, :]).astype(jnp.int32), axis=1)
        mine_dev = mine.reshape(devices, tok_rows, n_loc)
        before = jnp.tril(jnp.ones((tok_rows, tok_rows), BF), -1)
        rank = jnp.einsum('ut,dte->due', before, mine_dev.astype(BF), preferred_element_type=F32).astype(jnp.int32)
        slot = (jnp.arange(devices, dtype=jnp.int32) % per_block)[:, None, None] * cap + rank
        slot = jnp.where(mine_dev > 0, slot, -1).reshape(blocks, per_block * tok_rows, n_loc)
        n_slot = per_block * cap
        pick = jnp.arange(n_slot, dtype=jnp.int32)[None, None, :, None] == slot.transpose(0, 2, 1)[:, :, None, :]
        sel = pick.astype(BF)

        logits = jnp.dot(x_all, w_router, preferred_element_type=F32)
        probs = jax.nn.softmax(logits, axis=-1)
        gate_loc = GATE_SCALE * lax.dynamic_slice_in_dim(probs, me * n_loc, n_loc, 1)
        gate_t = gate_loc.reshape(blocks, per_block * tok_rows, n_loc).transpose(0, 2, 1)
        gate_slot = jnp.sum(jnp.where(pick, gate_t[:, :, None, :], 0.0), axis=-1)

        rows = dot('hest,htd->hesd', sel, x_all.reshape(blocks, per_block * tok_rows, dim)).astype(BF)
        gate_pre = dot('hesd,edf->hesf', rows, w_gate).astype(BF)
        up_pre = dot('hesd,edf->hesf', rows, w_up).astype(BF)
        hidden = swiglu_act(gate_pre.astype(F32), up_pre.astype(F32)).astype(BF)
        hidden_other = zswap(hidden)
        dy_rows = dot('hest,htd->hesd', sel, dy_all.reshape(blocks, per_block * tok_rows, dim)).astype(BF)
        d_out = (dy_rows.astype(F32) * gate_slot[..., None]).astype(BF)
        d_hidden = dot('hesd,efd->hesf', d_out, w_down).astype(BF)
        d_gate_pre, d_up_pre = act_grads(gate_pre, up_pre, d_hidden)

        w1_other = lax.dynamic_slice_in_dim(w_gate, other_col, half, 1)
        w3_other = lax.dynamic_slice_in_dim(w_up, other_col, half, 1)
        w1_mine = lax.dynamic_slice_in_dim(w_gate, my_col, half, 1)
        w3_mine = lax.dynamic_slice_in_dim(w_up, my_col, half, 1)
        width = half // COL_CHUNKS
        dx_parts = []
        gots = [w2_other, hidden_other]
        for j in range(COL_CHUNKS):
            c = slice(j * width, (j + 1) * width)
            give = dot('hesf,edf->hesd', d_gate_pre, w1_other[:, c]) + dot('hesf,edf->hesd', d_up_pre, w3_other[:, c])
            got = zswap(after(give, gots[-2]))
            gots.append(got)
            own = dot('hesf,edf->hesd', d_gate_pre, w1_mine[:, c]) + dot('hesf,edf->hesd', d_up_pre, w3_mine[:, c])
            d_rows = (own + got).astype(BF)
            dense = dot('hest,hesd->htd', sel, d_rows).reshape(tokens, width)
            dx_parts.append(reduce_rows(dense))
        dx_routed = jnp.concatenate(dx_parts, axis=1)

        w2_mine = lax.dynamic_slice_in_dim(w_down, my_col, half, 2)
        out_rows = (dot('hesf,efd->hesd', hidden, w2_mine) + dot('hesf,efd->hesd', hidden_other, w2_other)).astype(BF)
        dy_mine = lax.dynamic_slice_in_dim(dy_rows, my_col, half, 3)
        d_gate_slot = jnp.sum(out_rows.astype(F32) * dy_mine.astype(F32), axis=-1)
        d_gate_t = jnp.sum(jnp.where(pick, d_gate_slot[..., None], 0.0), axis=2).transpose(0, 2, 1).reshape(tokens, n_loc)
        d_gate_wide = lax.dynamic_update_slice_in_dim(jnp.zeros((tokens, experts), F32), d_gate_t, me * n_loc, 1)
        hi, mid, low = three_parts(out_rows.astype(F32) * gate_slot[..., None])
        y_dense = dot('hest,hesd->htd', sel, hi) + dot('hest,hesd->htd', sel, mid) + dot('hest,hesd->htd', sel, low)
        y_wide = jnp.concatenate([y_dense.reshape(tokens, half), d_gate_wide], axis=1)
        y_wide = reduce_rows(y_wide)
        y_sum, dg_sum = y_wide[:, :half], y_wide[:, half:]
        d_gates = dg_sum + zswap(dg_sum)

        sg_pre = jnp.dot(x_all, ws_gate, preferred_element_type=F32).astype(BF)
        su_pre = jnp.dot(x_all, ws_up, preferred_element_type=F32).astype(BF)
        s_hidden = swiglu_act(sg_pre.astype(F32), su_pre.astype(F32)).astype(BF)
        ds_hidden = dot('td,fd->tf', dy_all, ws_down).astype(BF)
        dsg_pre, dsu_pre = act_grads(sg_pre, su_pre, ds_hidden)
        ds_down = dot('tf,td->fd', s_hidden, dy_all)
        ds_gate = dot('td,tf->df', x_all, dsg_pre)
        ds_up = dot('td,tf->df', x_all, dsu_pre)

        s_part = jnp.dot(s_hidden[:grp], ws_down, preferred_element_type=F32)
        dxs_part = dot('tf,df->td', dsg_pre[:grp], ws_gate) + dot('tf,df->td', dsu_pre[:grp], ws_up)
        both = jnp.stack([s_part, dxs_part])
        got_shared = zswap(lax.dynamic_slice_in_dim(both, other_col, half, 2))
        shared = lax.dynamic_slice_in_dim(both, my_col, half, 2) + got_shared

        d_w_down = dot('hesf,hesd->efd', hidden, d_out)
        d_w_gate = dot('hesd,hesf->edf', rows, d_gate_pre)
        d_w_up = dot('hesd,hesf->edf', rows, d_up_pre)

        p_own = probs[:grp]
        d_scores = GATE_SCALE * d_gates
        d_logits = p_own * (d_scores - jnp.sum(p_own * d_scores, axis=-1, keepdims=True))
        d_router = dot('td,te->de', x_all[:grp], d_logits)
        for bit in (1, 2, 4):
            d_router = d_router + ep_swap(d_router, bit)
        wr_mine = lax.dynamic_slice_in_dim(w_router, my_col, half, 0)
        dx_router = dot('te,de->td', d_logits, wr_mine)

        y_half = (shared[0] + y_sum).astype(BF)
        dx_half = (dx_router + shared[1] + dx_routed).astype(BF)

        def to_owner(v):
            v = v.reshape(tp_size, tok_rows, half)
            keep = lax.dynamic_index_in_dim(v, z, 0, keepdims=False)
            got = zswap(lax.dynamic_index_in_dim(v, 1 - z, 0, keepdims=False))
            return jnp.where(z == 0, jnp.concatenate([keep, got], axis=-1), jnp.concatenate([got, keep], axis=-1))

        return to_owner(y_half), to_owner(dx_half), d_router, d_w_gate, d_w_up, d_w_down, ds_gate, ds_up, ds_down

    tok_spec = P(('ep', 'tp'), None)
    in_specs = (tok_spec, tok_spec, P(None, None), P('ep', None, 'tp'), P('ep', None, 'tp'), P('ep', 'tp', None), P(None, 'tp'), P(None, 'tp'), P('tp', None), tok_spec)
    out_specs = (tok_spec, tok_spec, P(None, None), P('ep', None, 'tp'), P('ep', None, 'tp'), P('ep', 'tp', None), P(None, 'tp'), P(None, 'tp'), P('tp', None))
    return jax.shard_map(device_step, mesh=mesh, in_specs=in_specs, out_specs=out_specs, check_vma=False)
```
